32 devices in a mesh: chain: 8 (over y, x, core), lane: 4 (over z).
Axes of the slice: x: 2, y: 2, z: 4, core: 2. Of those that a mesh axis runs over, the one named last changes fastest.
Arguments:
- fiedler: float32 [16, 96, 128, 128], P(None, 'chain', 'lane'), may hold values from -6 to 6
- side_labels: int32 [96, 128, 128], P('chain', 'lane'), may hold values from 0 to 1, as said below
Outputs:
- squared_image: float32 [16, 120, 128, 128], P(None, 'chain', 'lane')
- gram_blocks: float32 [2, 16, 16], replicated
The draws below stay inside these ranges and needn't reach their ends.
Inputs may be any that keep to these rules, and one draw needn't show every extreme that they name: `side_labels`: along every line of the first dimension (fixed second and third index) the vertices of side 0 form one run of planes [a, b) with 18 <= a <= 30 and 66 <= b <= 78; all other vertices are of side 1.
All inputs are finite; a program needn't handle non-finite values.
Results may differ from the reference program's by a relative error of at most 0.0001.
Values sent between devices are 32-bit elements; how exact they have to be, the bound alone decides.
A program may use at most 128 MiB of HBM per device.

```python
import jax
import jax.numpy as jnp
from jax import lax

K = 16
NZ = 128
MARGIN = 6
NX = 96
NY = 128
BAND = 60


def draw_side_labels(key, part):
    key_low = jax.random.fold_in(key, 11)
    key_high = jax.random.fold_in(key, 23)
    shift_low = jax.random.randint(key_low, (NY, NZ), -MARGIN, MARGIN + 1)
    shift_high = jax.random.randint(key_high, (NY, NZ), -MARGIN, MARGIN + 1)
    planes = jnp.arange(NX, dtype=jnp.int32)[:, None, None]
    lower_edge = NX // 4 + shift_low
    upper_edge = 3 * NX // 4 + shift_high
    inside = (planes >= lower_edge[None]) & (planes < upper_edge[None])
    return jnp.where(inside, 0, 1).astype(jnp.int32)


def block_levels(key, extent, split, smallest, largest):
    def one(dim, blocks):
        draws = jax.random.uniform(jax.random.fold_in(jax.random.fold_in(key, 6), dim), (blocks,), jnp.float32, smallest / len(split), largest / len(split))
        return jnp.repeat(jnp.exp(draws), extent[dim] // blocks).reshape((-1,) + (1,) * (len(extent) - dim - 1))

    factor_of = one(*split[0])
    for cut in split[1:]:
        factor_of = factor_of * one(*cut)
    return factor_of


def bell_draw(stream_key, extent, spread, reach, split=(), held_as=jnp.bfloat16):
    array = spread * jax.random.normal(stream_key, extent, jnp.float32)
    if split:
        array = array * block_levels(stream_key, extent, split, -0.22, 0.18)
    return jnp.clip(array, -reach, reach).astype(held_as)


def setup_inputs(seed: int = 0) -> dict:
    key_of = jax.random.split(jax.random.key(seed), 3)
    fiedler = bell_draw(key_of[0], (K, NX, NY, NZ), 1.0, 6.0, ((1, 8), (2, 4)), jnp.float32)
    side_labels = draw_side_labels(jax.random.fold_in(key_of[2], 71), 0)
    return dict(fiedler=fiedler, side_labels=side_labels)


def neighbour_sum(field):
    padded = jnp.pad(field, ((0, 0), (1, 1), (0, 0), (0, 0)))
    total = padded[:, :-2] + padded[:, 2:]
    total = total + jnp.roll(field, 1, 2) + jnp.roll(field, -1, 2)
    total = total + jnp.roll(field, 1, 3) + jnp.roll(field, -1, 3)
    return total


def reference(fiedler, side_labels):
    images = []
    grams = []
    for half_idx in range(2):
        start_plane = NX // 4 - MARGIN + half_idx * (NX // 2)
        rolled = jnp.roll(fiedler, -start_plane, axis=1)[:, :BAND]
        labels_band = jnp.roll(side_labels, -start_plane, axis=0)[:BAND]
        keep = labels_band == half_idx
        member = keep.astype(jnp.float32)[None]
        moved = jnp.where(keep[None], rolled, jnp.float32(0.0))
        degree = neighbour_sum(member)
        once_applied = member * (degree * moved - neighbour_sum(moved)) / 6.0
        twice_applied = member * (degree * once_applied - neighbour_sum(once_applied)) / 6.0
        gram = jnp.einsum("kpyz,lpyz->kl", once_applied, once_applied, precision=lax.Precision.HIGHEST)
        images.append(twice_applied)
        grams.append(gram / (BAND * NY * NZ))
    joined = jnp.concatenate(images, axis=1)
    return jnp.roll(joined, BAND // 2, axis=1), jnp.stack(grams)
```

```python
import functools

import jax
import jax.numpy as jnp
import numpy as np
from jax import lax
from jax.experimental import pallas as pl
from jax.experimental.pallas import tpu as pltpu
from jax.sharding import PartitionSpec as P

REACH = 2


def band_plan(chain_count, plane_count):
    half_count = chain_count // 2
    band_planes = plane_count + plane_count // 4
    total_planes = plane_count * chain_count
    margin_planes = (band_planes - plane_count) * half_count // 2
    own_slot = np.zeros(chain_count, np.int32)
    bounds = np.zeros((2, chain_count), np.int32)
    sides = np.zeros(chain_count, np.int32)
    transfers = []
    for target in range(chain_count):
        relative = (target - chain_count // 4) % chain_count
        side = relative // half_count
        within = relative % half_count
        first = total_planes // 4 - margin_planes + side * (total_planes // 2) + within * band_planes - REACH
        slot = (target * plane_count - first + total_planes // 2) % total_planes - total_planes // 2
        low = REACH if within == 0 else 0
        high = band_planes + (REACH if within == half_count - 1 else 2 * REACH)
        own_slot[target], sides[target] = slot, side
        bounds[:, target] = low, high
        below, above = max(0, slot - low), max(0, high - slot - plane_count)
        assert below <= plane_count and above <= plane_count
        if below:
            transfers.append((below, (target - 1) % chain_count, target, 1))
        if above:
            transfers.append((above, (target + 1) % chain_count, target, 2))
    groups = []
    for count, source, target, way in sorted(transfers, reverse=True):
        for group in groups:
            if group["count"] == count and source not in group["sources"] and target not in group["targets"]:
                break
        else:
            group = dict(count=count, sources=[], targets=[], start=np.zeros(chain_count, np.int32),
                         arrives=np.full(chain_count, -1, np.int32))
            groups.append(group)
        group["sources"].append(source)
        group["targets"].append(target)
        group["start"][source] = plane_count - count if way == 1 else 0
        group["arrives"][target] = plane_count + own_slot[target] + (-count if way == 1 else plane_count)
    return band_planes, own_slot, bounds, sides, groups


def two_sided(field):
    return (
        pltpu.roll(field, 1, 0) + pltpu.roll(field, field.shape[0] - 1, 0)
        + pltpu.roll(field, 1, 1) + pltpu.roll(field, field.shape[1] - 1, 1)
    )


def laplace_kernel(counts, planes, lines, band, vectors, table, *refs):
    groups = len(counts)
    own, own_marks, edge, edge_marks = refs[:4]
    got = refs[4 : 4 + 4 * groups]
    image, gram, field, mark, scale, degree, once, kept = refs[4 + 4 * groups :]
    k = pl.program_id(0)
    window = band + 2 * REACH

    def place(dest, start, count, body, border):
        dest[pl.ds(start, count), 0:lines, :] = body
        dest[pl.ds(start, count), lines : lines + REACH, :] = border[:, 0:REACH]
        dest[pl.ds(start, count), lines + 8 - REACH : lines + 8, :] = border[:, REACH:]

    def gather(dest, body, border, which):
        place(dest, planes + table[0], planes, body, border)
        for g in range(groups):
            start = table[4 + g]

            @pl.when(start >= 0)
            def _():
                place(dest, start, counts[g], got[4 * g + which][0], got[4 * g + 2 + which][0])

    @pl.when(k == 0)
    def _():
        mark[...] = jnp.full(mark.shape, -1.0, jnp.float32)
        gather(mark, own_marks[...].astype(jnp.float32), edge_marks[0], 1)
        side = table[3].astype(jnp.float32)
        for s in range(window):
            inside = (s >= table[1]) & (s < table[2])
            here = jnp.where(inside, side, jnp.float32(-2.0))
            mark[planes + s] = (mark[planes + s] == here).astype(jnp.float32)
        for s in range(1, window - 1):
            at = planes + s
            total = mark[at - 1] + mark[at + 1] + two_sided(mark[at])
            scale[s] = mark[at] / 6.0
            degree[s] = mark[at] * total / 6.0

    gather(field, own[0], edge[0], 0)

    def moved(s):
        return jnp.where(mark[planes + s] > 0.5, field[planes + s], 0.0)

    before, here = moved(0), moved(1)
    for s in range(1, window - 1):
        after = moved(s + 1)
        value = degree[s] * here - scale[s] * (before + after + two_sided(here))
        once[s] = value
        if REACH <= s < window - REACH:
            kept[pl.ds((s - REACH) * lines * vectors + k, lines, stride=vectors), :] = value[0:lines]
        before, here = here, after
    for s in range(REACH, window - REACH):
        value = once[s]
        result = degree[s] * value - scale[s] * (once[s - 1] + once[s + 1] + two_sided(value))
        image[0, s - REACH] = result[0:lines]

    @pl.when(k == vectors - 1)
    def _():
        rows = 8 * vectors
        steps = band * lines // 8

        def add(step, total):
            block = kept[pl.ds(pl.multiple_of(step * rows, rows), rows), :]
            high = block.astype(jnp.bfloat16)
            low = (block - high.astype(jnp.float32)).astype(jnp.bfloat16)
            dot = functools.partial(
                lax.dot_general, dimension_numbers=(((1,), (1,)), ((), ())), preferred_element_type=jnp.float32
            )
            return total + dot(high, high) + (dot(high, low) + dot(low, high))

        total = lax.fori_loop(0, steps, add, jnp.zeros((rows, rows), jnp.float32), unroll=2)
        gram[...] = total


def per_device(fiedler, side_labels):
    chain_count, lane_count = lax.axis_size("chain"), lax.axis_size("lane")
    vectors, plane_count, lines, width = fiedler.shape
    band, own_slot, bounds, sides, groups = band_plan(chain_count, plane_count)
    me = lax.axis_index("chain")
    marks = side_labels.astype(jnp.float32)[None]

    def both(part):
        return jnp.concatenate([part(fiedler), part(marks)], axis=0)

    up = [(i, (i + 1) % lane_count) for i in range(lane_count)]
    down = [(j, i) for i, j in up]
    after = lax.ppermute(both(lambda a: a[:, :, :REACH]), "lane", down)
    before = lax.ppermute(both(lambda a: a[:, :, lines - REACH :]), "lane", up)
    edge = jnp.concatenate([after, before], axis=2)

    counts = tuple(group["count"] for group in groups)
    got, edges_got = [], []
    for group in groups:
        start = jnp.asarray(group["start"])[me]
        pairs = list(zip(group["sources"], group["targets"]))
        count = group["count"]
        cut = functools.partial(lax.dynamic_slice_in_dim, start_index=start, slice_size=count, axis=1)
        got.append(lax.ppermute(both(cut), "chain", pairs))
        edges_got.append(lax.ppermute(cut(edge), "chain", pairs))

    rows = np.stack([own_slot, bounds[0], bounds[1], sides] + [group["arrives"] for group in groups])
    table = jnp.asarray(rows)[:, me]

    def spec(shape, at):
        return pl.BlockSpec((1,) + shape[1:], lambda k, t: (k if at is None else at, 0, 0, 0))

    operands = [fiedler, side_labels, edge, edge]
    in_specs = [
        spec(fiedler.shape, None),
        pl.BlockSpec(side_labels.shape, lambda k, t: (0, 0, 0)),
        spec(edge.shape, None),
        spec(edge.shape, vectors),
    ]
    for body, border in zip(got, edges_got):
        operands += [body, body, border, border]
        in_specs += [spec(body.shape, None), spec(body.shape, vectors)]
        in_specs += [spec(border.shape, None), spec(border.shape, vectors)]
    window = band + 2 * REACH
    tall = lines + 8
    held = (plane_count * 2 + window, tall, width)
    image, wide = pl.pallas_call(
        functools.partial(laplace_kernel, counts, plane_count, lines, band, vectors),
        grid_spec=pltpu.PrefetchScalarGridSpec(
            num_scalar_prefetch=1,
            grid=(vectors,),
            in_specs=in_specs,
            out_specs=[
                pl.BlockSpec((1, band, lines, width), lambda k, t: (k, 0, 0, 0)),
                pl.BlockSpec((8 * vectors, 8 * vectors), lambda k, t: (0, 0)),
            ],
            scratch_shapes=[
                pltpu.VMEM(held, jnp.float32),
                pltpu.VMEM(held, jnp.float32),
                pltpu.VMEM((window, tall, width), jnp.float32),
                pltpu.VMEM((window, tall, width), jnp.float32),
                pltpu.VMEM((window, tall, width), jnp.float32),
                pltpu.VMEM((band * lines * vectors, width), jnp.float32),
            ],
        ),
        out_shape=[
            jax.ShapeDtypeStruct((vectors, band, lines, width), jnp.float32),
            jax.ShapeDtypeStruct((8 * vectors, 8 * vectors), jnp.float32),
        ],
        compiler_params=pltpu.CompilerParams(
            dimension_semantics=("arbitrary",), vmem_limit_bytes=48 * 1024 * 1024
        ),
        name="laplace",
    )(table, *operands)
    local = jnp.einsum("akal->kl", wide.reshape(8, vectors, 8, vectors))
    slots = band * (chain_count // 2) * lines * lane_count * width
    mine = jnp.arange(2, dtype=jnp.int32)[:, None, None] == jnp.asarray(sides)[me]
    blocks = jnp.where(mine, local[None] / slots, jnp.float32(0.0))
    return image, lax.psum(blocks, ("chain", "lane"))


def solution(mesh):
    return jax.shard_map(
        per_device,
        mesh=mesh,
        in_specs=(P(None, "chain", "lane", None), P("chain", "lane", None)),
        out_specs=(P(None, "chain", "lane", None), P()),
        check_vma=False,
    )
```

```python
import functools

import jax
import jax.numpy as jnp
import numpy as np
from jax import lax
from jax.experimental import pallas as pl
from jax.experimental.pallas import tpu as pltpu
from jax.sharding import PartitionSpec as P

REACH = 2


def band_plan(chain_count, plane_count):
    half_count = chain_count // 2
    band_planes = plane_count + plane_count // 4
    total_planes = plane_count * chain_count
    margin_planes = (band_planes - plane_count) * half_count // 2
    own_slot = np.zeros(chain_count, np.int32)
    bounds = np.zeros((2, chain_count), np.int32)
    sides = np.zeros(chain_count, np.int32)
    transfers = []
    for target in range(chain_count):
        relative = (target - chain_count // 4) % chain_count
        side = relative // half_count
        within = relative % half_count
        first = total_planes // 4 - margin_planes + side * (total_planes // 2) + within * band_planes - REACH
        slot = (target * plane_count - first + total_planes // 2) % total_planes - total_planes // 2
        low = REACH if within == 0 else 0
        high = band_planes + (REACH if within == half_count - 1 else 2 * REACH)
        own_slot[target], sides[target] = slot, side
        bounds[:, target] = low, high
        below, above = max(0, slot - low), max(0, high - slot - plane_count)
        assert below <= plane_count and above <= plane_count
        if below:
            transfers.append((below, (target - 1) % chain_count, target, 1))
        if above:
            transfers.append((above, (target + 1) % chain_count, target, 2))
    groups = []
    for count, source, target, way in sorted(transfers, reverse=True):
        for group in groups:
            if group["count"] == count and source not in group["sources"] and target not in group["targets"]:
                break
        else:
            group = dict(count=count, sources=[], targets=[], start=np.zeros(chain_count, np.int32),
                         arrives=np.full(chain_count, -1, np.int32))
            groups.append(group)
        group["sources"].append(source)
        group["targets"].append(target)
        group["start"][source] = plane_count - count if way == 1 else 0
        group["arrives"][target] = plane_count + own_slot[target] + (-count if way == 1 else plane_count)
    return band_planes, own_slot, bounds, sides, groups


def two_sided(field):
    return (
        pltpu.roll(field, 1, 0) + pltpu.roll(field, field.shape[0] - 1, 0)
        + pltpu.roll(field, 1, 1) + pltpu.roll(field, field.shape[1] - 1, 1)
    )


def laplace_kernel(counts, planes, lines, band, vectors, slots, table, *refs):
    groups = len(counts)
    own, own_marks, edge, edge_marks = refs[:4]
    got = refs[4 : 4 + 4 * groups]
    image, gram, field, mark, scale, degree, once, kept = refs[4 + 4 * groups :]
    k = pl.program_id(0)
    window = band + 2 * REACH

    def place(dest, start, count, body, border):
        dest[pl.ds(start, count), 0:lines, :] = body
        dest[pl.ds(start, count), lines : lines + REACH, :] = border[:, 0:REACH]
        dest[pl.ds(start, count), lines + 8 - REACH : lines + 8, :] = border[:, REACH:]

    def gather(dest, body, border, which):
        place(dest, planes + table[0], planes, body, border)
        for g in range(groups):
            start = table[4 + g]

            @pl.when(start >= 0)
            def _():
                place(dest, start, counts[g], got[4 * g + which][0], got[4 * g + 2 + which][0])

    @pl.when(k == 0)
    def _():
        mark[...] = jnp.full(mark.shape, -1.0, jnp.float32)
        gather(mark, own_marks[...].astype(jnp.float32), edge_marks[0], 1)
        side = table[3].astype(jnp.float32)
        for s in range(window):
            inside = (s >= table[1]) & (s < table[2])
            here = jnp.where(inside, side, jnp.float32(-2.0))
            mark[planes + s] = (mark[planes + s] == here).astype(jnp.float32)
        for s in range(1, window - 1):
            at = planes + s
            total = mark[at - 1] + mark[at + 1] + two_sided(mark[at])
            scale[s] = mark[at] / 6.0
            degree[s] = mark[at] * total / 6.0

    gather(field, own[0], edge[0], 0)

    def moved(s):
        return jnp.where(mark[planes + s] > 0.5, field[planes + s], 0.0)

    before, here = moved(0), moved(1)
    for s in range(1, window - 1):
        after = moved(s + 1)
        value = degree[s] * here - scale[s] * (before + after + two_sided(here))
        once[s] = value
        if REACH <= s < window - REACH:
            kept[pl.ds((s - REACH) * lines * vectors + k, lines, stride=vectors), :] = value[0:lines]
        before, here = here, after
    for s in range(REACH, window - REACH):
        value = once[s]
        result = degree[s] * value - scale[s] * (once[s - 1] + once[s + 1] + two_sided(value))
        image[0, s - REACH] = result[0:lines]

    @pl.when(k == vectors - 1)
    def _():
        rows = 8 * vectors
        steps = band * lines // 8

        def add(step, total):
            block = kept[pl.ds(pl.multiple_of(step * rows, rows), rows), :]
            high = block.astype(jnp.bfloat16)
            low = (block - high.astype(jnp.float32)).astype(jnp.bfloat16)
            dot = functools.partial(
                lax.dot_general, dimension_numbers=(((1,), (1,)), ((), ())), preferred_element_type=jnp.float32
            )
            return total + dot(high, high) + (dot(high, low) + dot(low, high))

        total = lax.fori_loop(0, steps, add, jnp.zeros((rows, rows), jnp.float32), unroll=2)
        row = lax.broadcasted_iota(jnp.int32, total.shape, 0) // vectors
        column = lax.broadcasted_iota(jnp.int32, total.shape, 1) // vectors
        total = jnp.where(row == column, total, 0.0)
        folded = total[0:vectors]
        for part in range(1, 8):
            folded = folded + total[part * vectors : (part + 1) * vectors]
        shift = rows // 2
        while shift >= vectors:
            folded = folded + pltpu.roll(folded, shift, 1)
            shift //= 2
        gram[...] = folded / slots


def gram_sum_kernel(sides, lane_count, local, out, lane_got, total, chain_got, *sems):
    chain_count = len(sides)
    my_chain, my_lane = lax.axis_index("chain"), lax.axis_index("lane")
    barrier = pltpu.get_barrier_semaphore()
    for d in range(1, lane_count):
        pl.semaphore_signal(barrier, inc=1, device_id=(my_chain, (my_lane + d) % lane_count),
                            device_id_type=pl.DeviceIdType.MESH)
    for d in range(1, chain_count):
        pl.semaphore_signal(barrier, inc=1, device_id=((my_chain + d) % chain_count, my_lane),
                            device_id_type=pl.DeviceIdType.MESH)
    pl.semaphore_wait(barrier, lane_count + chain_count - 2)

    def gather(src, got, me, count, device, send, recv):
        def copy(d, slot):
            return pltpu.make_async_remote_copy(
                src_ref=src, dst_ref=got.at[slot], send_sem=send.at[d], recv_sem=recv.at[d],
                device_id=device((me + d) % count), device_id_type=pl.DeviceIdType.MESH,
            )

        for d in range(1, count):
            copy(d, me).start()
        got[me] = src[...]
        for d in range(1, count):
            copy(d, (me + count - d) % count).wait_recv()
        for d in range(1, count):
            copy(d, me).wait_send()

    gather(local, lane_got, my_lane, lane_count, lambda i: (my_chain, i), sems[0], sems[1])
    value = lane_got[0]
    for i in range(1, lane_count):
        value = value + lane_got[i]
    total[...] = value
    gather(total, chain_got, my_chain, chain_count, lambda i: (i, my_lane), sems[2], sems[3])
    for side in range(2):
        members = [c for c in range(chain_count) if sides[c] == side]
        value = chain_got[members[0]]
        for c in members[1:]:
            value = value + chain_got[c]
        out[side] = value


def per_device(fiedler, side_labels):
    chain_count, lane_count = lax.axis_size("chain"), lax.axis_size("lane")
    vectors, plane_count, lines, width = fiedler.shape
    band, own_slot, bounds, sides, groups = band_plan(chain_count, plane_count)
    me = lax.axis_index("chain")
    slots = band * (chain_count // 2) * lines * lane_count * width
    rows = np.stack(
        [own_slot, bounds[0], bounds[1], sides]
        + [group["arrives"] for group in groups]
        + [group["start"] for group in groups]
    )
    table = lax.optimization_barrier(jnp.asarray(rows.T)[me])
    marks = side_labels.astype(jnp.float32)[None]

    def both(part):
        return jnp.concatenate([part(fiedler), part(marks)], axis=0)

    up = [(i, (i + 1) % lane_count) for i in range(lane_count)]
    down = [(j, i) for i, j in up]
    after = lax.ppermute(both(lambda a: a[:, :, :REACH]), "lane", down)
    before = lax.ppermute(both(lambda a: a[:, :, lines - REACH :]), "lane", up)
    edge = jnp.concatenate([after, before], axis=2)

    counts = tuple(group["count"] for group in groups)
    got, edges_got = [], []
    for which, group in enumerate(groups):
        start = table[4 + len(groups) + which]
        pairs = list(zip(group["sources"], group["targets"]))
        count = group["count"]
        cut = functools.partial(lax.dynamic_slice_in_dim, start_index=start, slice_size=count, axis=1)
        got.append(lax.ppermute(both(cut), "chain", pairs))
        edges_got.append(lax.ppermute(cut(edge), "chain", pairs))

    def spec(shape, at):
        return pl.BlockSpec((1,) + shape[1:], lambda k, t: (k if at is None else at, 0, 0, 0))

    operands = [fiedler, side_labels, edge, edge]
    in_specs = [
        spec(fiedler.shape, None),
        pl.BlockSpec(side_labels.shape, lambda k, t: (0, 0, 0)),
        spec(edge.shape, None),
        spec(edge.shape, vectors),
    ]
    for body, border in zip(got, edges_got):
        operands += [body, body, border, border]
        in_specs += [spec(body.shape, None), spec(body.shape, vectors)]
        in_specs += [spec(border.shape, None), spec(border.shape, vectors)]
    window = band + 2 * REACH
    tall = lines + 8
    held = (plane_count * 2 + window, tall, width)
    image, wide = pl.pallas_call(
        functools.partial(laplace_kernel, counts, plane_count, lines, band, vectors, float(slots)),
        grid_spec=pltpu.PrefetchScalarGridSpec(
            num_scalar_prefetch=1,
            grid=(vectors,),
            in_specs=in_specs,
            out_specs=[
                pl.BlockSpec((1, band, lines, width), lambda k, t: (k, 0, 0, 0)),
                pl.BlockSpec((vectors, 8 * vectors), lambda k, t: (0, 0)),
            ],
            scratch_shapes=[
                pltpu.VMEM(held, jnp.float32),
                pltpu.VMEM(held, jnp.float32),
                pltpu.VMEM((window, tall, width), jnp.float32),
                pltpu.VMEM((window, tall, width), jnp.float32),
                pltpu.VMEM((window, tall, width), jnp.float32),
                pltpu.VMEM((band * lines * vectors, width), jnp.float32),
            ],
        ),
        out_shape=[
            jax.ShapeDtypeStruct((vectors, band, lines, width), jnp.float32),
            jax.ShapeDtypeStruct((vectors, 8 * vectors), jnp.float32),
        ],
        compiler_params=pltpu.CompilerParams(
            dimension_semantics=("arbitrary",), vmem_limit_bytes=48 * 1024 * 1024
        ),
        name="laplace",
    )(table, *operands)
    shape = wide.shape
    sums = pl.pallas_call(
        functools.partial(gram_sum_kernel, tuple(int(side) for side in sides), lane_count),
        out_shape=jax.ShapeDtypeStruct((2,) + shape, jnp.float32),
        in_specs=[pl.BlockSpec(memory_space=pltpu.VMEM)],
        out_specs=pl.BlockSpec(memory_space=pltpu.VMEM),
        scratch_shapes=[
            pltpu.VMEM((lane_count,) + shape, jnp.float32),
            pltpu.VMEM(shape, jnp.float32),
            pltpu.VMEM((chain_count,) + shape, jnp.float32),
            pltpu.SemaphoreType.DMA((lane_count,)),
            pltpu.SemaphoreType.DMA((lane_count,)),
            pltpu.SemaphoreType.DMA((chain_count,)),
            pltpu.SemaphoreType.DMA((chain_count,)),
        ],
        compiler_params=pltpu.CompilerParams(collective_id=0, has_side_effects=True),
        name="gram_sum",
    )(wide)
    return image, sums[:, :, :vectors]


def solution(mesh):
    return jax.shard_map(
        per_device,
        mesh=mesh,
        in_specs=(P(None, "chain", "lane", None), P("chain", "lane", None)),
        out_specs=(P(None, "chain", "lane", None), P()),
        check_vma=False,
    )
```
